32 devices in a mesh: expert: 16 (over z, y, x), shard: 2 (over core).
Axes of the slice: x: 2, y: 2, z: 4, core: 2. Of those that a mesh axis runs over, the one named last changes fastest.
Arguments:
- w_gate: float32 [64, 2048, 1024], P('expert', 'shard'), may hold values from -0.125 to 0.125
- avg_gate: float32 [64, 2048, 1024], P('expert', 'shard'), may hold values from -0.125 to 0.125
- w_up: float32 [64, 2048, 1024], P('expert', 'shard'), may hold values from -0.125 to 0.125
- avg_up: float32 [64, 2048, 1024], P('expert', 'shard'), may hold values from -0.125 to 0.125
- mix_share: float32 [64], P('expert'), may hold values from 0.2 to 0.8
- router_weight: float32 [2048, 64], P('shard', 'expert'), may hold values from -0.125 to 0.125
- router_gain: float32 [2048], P('shard'), may hold values from 0.25 to 1.75
Outputs:
- serve_gate: bfloat16 [64, 1024, 2048], P('expert')
- serve_up: bfloat16 [64, 1024, 2048], P('expert')
- serve_router: bfloat16 [2048, 64], replicated
The draws below stay inside these ranges and needn't reach their ends.
All inputs are finite; a program needn't handle non-finite values.
Results may differ from the reference program's by a relative error of at most 0.001.
Values may be sent and summed in bfloat16 or wider, within the bound.
A program may use at most 192 MiB of HBM per device.

```python
import jax
import jax.numpy as jnp

EXPERTS = 64
D_MODEL = 2048
D_EXPERT = 1024


def levels(own_key, dims, pieces, low, top_value):
    level, own = 1.0, jax.random.fold_in(own_key, 6)
    for position, parts in pieces:
        draws = jnp.exp(jax.random.uniform(jax.random.fold_in(own, position), (parts,), jnp.float32, low / len(pieces), top_value / len(pieces)))
        level = level * jnp.repeat(draws, dims[position] // parts).reshape([-1 if axis == position else 1 for axis in range(len(dims))])
    return level


def gaussian(key, extent, scale, most, cuts=(), kind=jnp.bfloat16):
    level = levels(key, extent, cuts, -0.22, 0.18) if cuts else 1.0
    values = jax.random.normal(key, extent, jnp.float32) * scale * level
    return jnp.minimum(jnp.maximum(values, -most), most).astype(kind)


def setup_inputs(seed: int = 0) -> dict:
    streams_of = jax.random.split(jax.random.key(seed), 8)
    return {
        "w_gate": gaussian(streams_of[0], (EXPERTS, D_MODEL, D_EXPERT), D_MODEL ** -0.5, 0.125, ((0, 16), (1, 2)), jnp.float32),
        "avg_gate": gaussian(streams_of[1], (EXPERTS, D_MODEL, D_EXPERT), D_MODEL ** -0.5, 0.125, ((0, 16), (1, 2)), jnp.float32),
        "w_up": gaussian(streams_of[2], (EXPERTS, D_MODEL, D_EXPERT), D_MODEL ** -0.5, 0.125, ((0, 16), (1, 2)), jnp.float32),
        "avg_up": gaussian(streams_of[3], (EXPERTS, D_MODEL, D_EXPERT), D_MODEL ** -0.5, 0.125, ((0, 16), (1, 2)), jnp.float32),
        "mix_share": jnp.clip(0.2 + 0.6 * jax.random.uniform(streams_of[4], (EXPERTS,), jnp.float32) ** levels(streams_of[4], (EXPERTS,), ((0, 16),), -0.2, 0.2), 0.2, 0.8),
        "router_weight": gaussian(streams_of[5], (D_MODEL, EXPERTS), D_MODEL ** -0.5, 0.125, ((0, 2), (1, 16)), jnp.float32),
        "router_gain": jnp.clip(1.0 + 0.15 * jax.random.normal(streams_of[6], (D_MODEL,), jnp.float32), 0.25, 1.75),
    }


def reference(w_gate, avg_gate, w_up, avg_up, mix_share, router_weight, router_gain):
    fresh_gate = mix_share[:, None, None] * w_gate + (1.0 - mix_share[:, None, None]) * avg_gate
    fresh_up = mix_share[:, None, None] * w_up + (1.0 - mix_share[:, None, None]) * avg_up
    serve_gate = fresh_gate.astype(jnp.bfloat16)
    serve_gate = jnp.transpose(serve_gate, (0, 2, 1))
    serve_up = fresh_up.astype(jnp.bfloat16)
    serve_up = jnp.transpose(serve_up, (0, 2, 1))
    serve_router = (router_weight * router_gain[:, None]).astype(jnp.bfloat16)
    return serve_gate, serve_up, serve_router
```

```python
import functools

import jax
import jax.numpy as jnp
from jax import lax
from jax.experimental import pallas as pl
from jax.experimental.pallas import tpu as pltpu
from jax.sharding import PartitionSpec as P

MESH = pl.DeviceIdType.MESH
SLOTS = 4
ROWS = 256


def mix_kernel(peers, shards, rows, with_router, *refs):
    if with_router:
        (w_ref, avg_ref, mix_ref, weight_ref, gain_ref, out_ref, router_ref,
         w_buf, avg_buf, in_sem, send_sem, recv_sem,
         stage, total, hop_send, hop_recv, row_send, row_recv) = refs
    else:
        (w_ref, avg_ref, mix_ref, out_ref,
         w_buf, avg_buf, in_sem, send_sem, recv_sem) = refs
    me, at = lax.axis_index("shard"), lax.axis_index("expert")
    experts, depth, _ = w_ref.shape
    per = depth // rows
    pieces = experts * per

    def load(i):
        slot = lax.rem(i, SLOTS)
        expert, row = lax.div(i, per), pl.multiple_of(lax.rem(i, per) * rows, rows)
        return [
            pltpu.make_async_copy(src.at[expert, pl.ds(row, rows), :], buf.at[slot], in_sem.at[n, slot])
            for n, (src, buf) in enumerate(((w_ref, w_buf), (avg_ref, avg_buf)))
        ]

    def block(i, owner):
        expert = lax.div(i, per)
        column = pl.multiple_of(owner * depth + lax.rem(i, per) * rows, rows)
        return out_ref.at[expert, :, pl.ds(column, rows)]

    def exchange(i, owner, k):
        return pltpu.make_async_remote_copy(
            src_ref=block(i, owner), dst_ref=block(i, owner),
            send_sem=send_sem.at[k - 1, i], recv_sem=recv_sem.at[k - 1, i],
            device_id={"shard": lax.rem(me + k, shards)}, device_id_type=MESH,
        )

    for i in range(min(SLOTS, pieces)):
        for copy in load(i):
            copy.start()

    barrier = pltpu.get_barrier_semaphore()
    for k in range(1, shards):
        pl.semaphore_signal(barrier, inc=1, device_id={"shard": lax.rem(me + k, shards)}, device_id_type=MESH)
    if with_router:
        @pl.loop(1, peers)
        def _(k):
            pl.semaphore_signal(barrier, inc=1, device_id={"expert": lax.rem(at + k, peers)}, device_id_type=MESH)
    pl.semaphore_wait(barrier, shards - 1 + (peers - 1 if with_router else 0))

    if with_router:
        mine = pl.ds(pl.multiple_of(me * depth, depth), depth)
        stage[at, :, mine] = (weight_ref[...] * gain_ref[...]).astype(jnp.bfloat16)

        def hop(k):
            return pltpu.make_async_remote_copy(
                src_ref=stage.at[at, :, mine], dst_ref=stage.at[at, :, mine],
                send_sem=hop_send.at[k - 1], recv_sem=hop_recv.at[k - 1],
                device_id={"expert": lax.rem(at + k, peers)}, device_id_type=MESH,
            )

        def hop_in(k):
            source = lax.rem(at + peers - k, peers)
            return pltpu.make_async_remote_copy(
                src_ref=stage.at[source, :, mine], dst_ref=stage.at[source, :, mine],
                send_sem=hop_send.at[k - 1], recv_sem=hop_recv.at[k - 1],
                device_id={"expert": lax.rem(at + k, peers)}, device_id_type=MESH,
            )

        @pl.loop(1, peers)
        def _(k):
            hop(k).start()

    @pl.loop(0, pieces)
    def _(i):
        slot = lax.rem(i, SLOTS)
        for copy in load(i):
            copy.wait()
        share = mix_ref[lax.div(i, per)]
        fresh = share * w_buf[slot] + (1.0 - share) * avg_buf[slot]
        block(i, me)[...] = jnp.transpose(fresh.astype(jnp.bfloat16))
        for k in range(1, shards):
            exchange(i, me, k).start()

        @pl.when(i + SLOTS < pieces)
        def _():
            for copy in load(i + SLOTS):
                copy.start()

    if with_router:
        @pl.loop(1, peers)
        def _(k):
            hop(k).wait_send()
            hop_in(k).wait_recv()

        def rows_to(owner, k):
            columns = pl.ds(pl.multiple_of(owner * depth, depth), depth)
            return pltpu.make_async_remote_copy(
                src_ref=stage.at[:, :, columns], dst_ref=stage.at[:, :, columns],
                send_sem=row_send.at[k - 1], recv_sem=row_recv.at[k - 1],
                device_id={"shard": lax.rem(me + k, shards)}, device_id_type=MESH,
            )

        for k in range(1, shards):
            rows_to(me, k).start()
        for k in range(1, shards):
            rows_to(me, k).wait_send()
            rows_to(lax.rem(me + shards - k, shards), k).wait_recv()
        held = stage.shape[1]
        for e in range(peers):
            total[e * held:(e + 1) * held, :] = stage[e].astype(jnp.float32)
        router_ref[...] = total[...].astype(jnp.bfloat16)

    @pl.loop(0, pieces)
    def _(i):
        for k in range(1, shards):
            exchange(i, me, k).wait_send()
            exchange(i, lax.rem(me + shards - k, shards), k).wait_recv()


def mix(mesh, w, avg, share, router=None):
    peers, shards = mesh.shape["expert"], mesh.shape["shard"]
    experts, depth, width = w.shape
    rows = min(ROWS, depth)
    pieces = experts * (depth // rows)
    others = max(shards - 1, 1)
    any_spec = pl.BlockSpec(memory_space=pltpu.HBM)
    vmem_spec = pl.BlockSpec(memory_space=pltpu.VMEM)
    out_shape = [pltpu.VMEM((experts, width, shards * depth), jnp.bfloat16)]
    in_specs = [any_spec, any_spec, pl.BlockSpec(memory_space=pltpu.SMEM)]
    scratch = [
        pltpu.VMEM((SLOTS, rows, width), jnp.float32),
        pltpu.VMEM((SLOTS, rows, width), jnp.float32),
        pltpu.SemaphoreType.DMA((2, SLOTS)),
        pltpu.SemaphoreType.DMA((others, pieces)),
        pltpu.SemaphoreType.DMA((others, pieces)),
    ]
    args = tuple(pltpu.with_memory_space_constraint(x, pltpu.HBM) for x in (w, avg)) + (share,)
    if router is not None:
        args += router
        in_specs += [vmem_spec, vmem_spec]
        out_shape += [pltpu.VMEM((peers * experts, shards * depth), jnp.bfloat16)]
        scratch += [
            pltpu.VMEM((peers, experts, shards * depth), jnp.bfloat16),
            pltpu.VMEM((peers * experts, shards * depth), jnp.float32),
            pltpu.SemaphoreType.DMA((peers,)),
            pltpu.SemaphoreType.DMA((peers,)),
            pltpu.SemaphoreType.DMA((others,)),
            pltpu.SemaphoreType.DMA((others,)),
        ]
    return pl.pallas_call(
        functools.partial(mix_kernel, peers, shards, rows, router is not None),
        out_shape=out_shape,
        in_specs=in_specs,
        out_specs=[vmem_spec] * len(out_shape),
        scratch_shapes=scratch,
        compiler_params=pltpu.CompilerParams(
            collective_id=0 if router is not None else 1,
            has_side_effects=True,
            vmem_limit_bytes=20 * 2**20,
        ),
    )(*args)


def solution(mesh):
    def local(w_gate, avg_gate, w_up, avg_up, mix_share, router_weight, router_gain):
        serve_gate, router = mix(
            mesh, w_gate, avg_gate, mix_share, (router_weight.T, router_gain[None, :])
        )
        serve_up, = mix(mesh, w_up, avg_up, mix_share)
        return serve_gate, serve_up, router.T

    return jax.shard_map(
        local,
        mesh=mesh,
        in_specs=(
            P("expert", "shard", None),
            P("expert", "shard", None),
            P("expert", "shard", None),
            P("expert", "shard", None),
            P("expert"),
            P("shard", "expert"),
            P("shard"),
        ),
        out_specs=(P("expert", None, None), P("expert", None, None), P()),
        check_vma=False,
    )
```

```python
import functools

import jax
import jax.numpy as jnp
from jax import lax
from jax.experimental import pallas as pl
from jax.experimental.pallas import tpu as pltpu
from jax.sharding import PartitionSpec as P

MESH = pl.DeviceIdType.MESH
SLOTS = 4
SIZE = 256
BY_COLUMN = True
CUTS = 8


def mix_kernel(peers, shards, size, *refs):
    (w_gate, avg_gate, w_up, avg_up, mix_ref, weight_ref, gain_ref,
     gate_ref, up_ref, router_ref,
     w_buf, avg_buf, in_sem, send_sem, recv_sem,
     stage, total, hop_send, hop_recv, row_send, row_recv) = refs
    me, at = lax.axis_index("shard"), lax.axis_index("expert")
    experts, depth, width = w_gate.shape
    per = (width if BY_COLUMN else depth) // size
    pieces = experts * per
    sources, outs = ((w_gate, avg_gate), (w_up, avg_up)), (gate_ref, up_ref)

    def load(m, i):
        slot = lax.rem(i, SLOTS)
        expert, start = lax.div(i, per), pl.multiple_of(lax.rem(i, per) * size, size)
        def part(src):
            return src.at[expert, :, pl.ds(start, size)] if BY_COLUMN else src.at[expert, pl.ds(start, size), :]
        return [
            pltpu.make_async_copy(part(src), buf.at[slot], in_sem.at[n, slot])
            for n, (src, buf) in enumerate(zip(sources[m], (w_buf, avg_buf)))
        ]

    def block(m, i, owner):
        expert, start = lax.div(i, per), lax.rem(i, per) * size
        if BY_COLUMN:
            column = pl.multiple_of(owner * depth, depth)
            return outs[m].at[expert, pl.ds(pl.multiple_of(start, size), size), pl.ds(column, depth)]
        return outs[m].at[expert, :, pl.ds(pl.multiple_of(owner * depth + start, size), size)]

    def exchange(m, i, owner, k):
        return pltpu.make_async_remote_copy(
            src_ref=block(m, i, owner), dst_ref=block(m, i, owner),
            send_sem=send_sem.at[m, k - 1, i], recv_sem=recv_sem.at[m, k - 1, i],
            device_id={"shard": lax.rem(me + k, shards)}, device_id_type=MESH,
        )

    for i in range(min(SLOTS, pieces)):
        for copy in load(0, i):
            copy.start()

    barrier = pltpu.get_barrier_semaphore()
    for k in range(1, shards):
        pl.semaphore_signal(barrier, inc=1, device_id={"shard": lax.rem(me + k, shards)}, device_id_type=MESH)
    if True:
        @pl.loop(1, peers)
        def _(k):
            pl.semaphore_signal(barrier, inc=1, device_id={"expert": lax.rem(at + k, peers)}, device_id_type=MESH)
    pl.semaphore_wait(barrier, shards - 1 + peers - 1)

    if True:
        mine = pl.ds(pl.multiple_of(me * depth, depth), depth)
        stage[at, :, mine] = (weight_ref[...] * gain_ref[...]).astype(jnp.bfloat16)

        def hop(k):
            return pltpu.make_async_remote_copy(
                src_ref=stage.at[at, :, mine], dst_ref=stage.at[at, :, mine],
                send_sem=hop_send.at[k - 1], recv_sem=hop_recv.at[k - 1],
                device_id={"expert": lax.rem(at + k, peers)}, device_id_type=MESH,
            )

        def hop_in(k):
            source = lax.rem(at + peers - k, peers)
            return pltpu.make_async_remote_copy(
                src_ref=stage.at[source, :, mine], dst_ref=stage.at[source, :, mine],
                send_sem=hop_send.at[k - 1], recv_sem=hop_recv.at[k - 1],
                device_id={"expert": lax.rem(at + k, peers)}, device_id_type=MESH,
            )

        @pl.loop(1, peers)
        def _(k):
            hop(k).start()

    for m in range(2):
        @pl.loop(0, pieces)
        def _(i):
            slot = lax.rem(i, SLOTS)
            for copy in load(m, i):
                copy.wait()
            share = mix_ref[lax.div(i, per)]
            fresh = share * w_buf[slot] + (1.0 - share) * avg_buf[slot]
            block(m, i, me)[...] = jnp.transpose(fresh.astype(jnp.bfloat16))
            for k in range(1, shards):
                exchange(m, i, me, k).start()

            @pl.when(i + SLOTS < pieces)
            def _():
                for copy in load(m, i + SLOTS):
                    copy.start()

            if m == 0:
                @pl.when(i + SLOTS >= pieces)
                def _():
                    for copy in load(1, i + SLOTS - pieces):
                        copy.start()

    if True:
        @pl.loop(1, peers)
        def _(k):
            hop(k).wait_send()
            hop_in(k).wait_recv()

        def rows_to(owner, k):
            columns = pl.ds(pl.multiple_of(owner * depth, depth), depth)
            return pltpu.make_async_remote_copy(
                src_ref=stage.at[:, :, columns], dst_ref=stage.at[:, :, columns],
                send_sem=row_send.at[k - 1], recv_sem=row_recv.at[k - 1],
                device_id={"shard": lax.rem(me + k, shards)}, device_id_type=MESH,
            )

        for k in range(1, shards):
            rows_to(me, k).start()
        for k in range(1, shards):
            rows_to(me, k).wait_send()
            rows_to(lax.rem(me + shards - k, shards), k).wait_recv()
        held = stage.shape[1]
        for e in range(peers):
            total[e * held:(e + 1) * held, :] = stage[e].astype(jnp.float32)
        router_ref[...] = total[...].astype(jnp.bfloat16)

    for m in range(2):
        @pl.loop(0, pieces)
        def _(i):
            for k in range(1, shards):
                exchange(m, i, me, k).wait_send()
                exchange(m, i, lax.rem(me + shards - k, shards), k).wait_recv()


def mix(mesh, sources, share, weight, gain):
    peers, shards = mesh.shape["expert"], mesh.shape["shard"]
    experts, depth, width = sources[0].shape
    span = width if BY_COLUMN else depth
    size = min(SIZE, span)
    pieces = experts * (span // size)
    assert pieces % SLOTS == 0
    others = max(shards - 1, 1)
    hbm_spec = pl.BlockSpec(memory_space=pltpu.HBM)
    vmem_spec = pl.BlockSpec(memory_space=pltpu.VMEM)
    buffer = pltpu.VMEM((SLOTS, depth, size) if BY_COLUMN else (SLOTS, size, width), jnp.float32)
    half = pltpu.VMEM((experts, width, shards * depth), jnp.bfloat16)
    return pl.pallas_call(
        functools.partial(mix_kernel, peers, shards, size),
        out_shape=[half, half, pltpu.VMEM((peers * experts, shards * depth), jnp.bfloat16)],
        in_specs=[hbm_spec] * 4 + [pl.BlockSpec(memory_space=pltpu.SMEM), vmem_spec, vmem_spec],
        out_specs=[vmem_spec] * 3,
        scratch_shapes=[
            buffer,
            buffer,
            pltpu.SemaphoreType.DMA((2, SLOTS)),
            pltpu.SemaphoreType.DMA((2, others, pieces)),
            pltpu.SemaphoreType.DMA((2, others, pieces)),
            pltpu.VMEM((peers, experts, shards * depth), jnp.bfloat16),
            pltpu.VMEM((peers * experts, shards * depth), jnp.float32),
            pltpu.SemaphoreType.DMA((peers,)),
            pltpu.SemaphoreType.DMA((peers,)),
            pltpu.SemaphoreType.DMA((others,)),
            pltpu.SemaphoreType.DMA((others,)),
        ],
        compiler_params=pltpu.CompilerParams(
            collective_id=0, has_side_effects=True, vmem_limit_bytes=12 * 2**20
        ),
    )(*(pltpu.with_memory_space_constraint(x, pltpu.HBM) for x in sources), share, weight, gain)


def store_kernel(*refs):
    count = (len(refs) - 1) // 2
    copies = []
    for n in range(count):
        source, target = refs[n], refs[count + n]
        step = max(source.shape[0] // CUTS, 1) if len(source.shape) == 2 else source.shape[0]
        if len(source.shape) == 3:
            step = source.shape[1] // 2
            for e in range(source.shape[0]):
                for r in range(2):
                    copies.append((source.at[e, pl.ds(r * step, step), :], target.at[e, pl.ds(r * step, step), :]))
        else:
            copies.append((source, target))
    started = [pltpu.make_async_copy(a, b, refs[-1].at[n]) for n, (a, b) in enumerate(copies)]
    for copy in started:
        copy.start()
    for copy in started:
        copy.wait()


def store(*arrays):
    vmem_spec = pl.BlockSpec(memory_space=pltpu.VMEM)
    count = sum(2 * x.shape[0] if x.ndim == 3 else 1 for x in arrays)
    return pl.pallas_call(
        store_kernel,
        out_shape=[pltpu.HBM(x.shape, x.dtype) for x in arrays],
        in_specs=[vmem_spec] * len(arrays),
        out_specs=[pl.BlockSpec(memory_space=pltpu.HBM)] * len(arrays),
        scratch_shapes=[pltpu.SemaphoreType.DMA((count,))],
        compiler_params=pltpu.CompilerParams(vmem_limit_bytes=2**20),
    )(*arrays)


def solution(mesh):
    def local(w_gate, avg_gate, w_up, avg_up, mix_share, router_weight, router_gain):
        gate, up, router = mix(
            mesh, (w_gate, avg_gate, w_up, avg_up), mix_share, router_weight.T, router_gain[None, :]
        )
        gate, up, router = store(gate, up, router)
        return gate, up, router.T

    return jax.shard_map(
        local,
        mesh=mesh,
        in_specs=(
            P("expert", "shard", None),
            P("expert", "shard", None),
            P("expert", "shard", None),
            P("expert", "shard", None),
            P("expert"),
            P("shard", "expert"),
            P("shard"),
        ),
        out_specs=(P("expert", None, None), P("expert", None, None), P()),
        check_vma=False,
    )
```

```python
import functools

import jax
import jax.numpy as jnp
from jax import lax
from jax.experimental import pallas as pl
from jax.experimental.pallas import tpu as pltpu
from jax.sharding import PartitionSpec as P

MESH = pl.DeviceIdType.MESH
SLOTS = 4
SIZE = 256
BY_COLUMN = True
EARLY = 2


def mix_kernel(peers, shards, size, plan, with_router, *refs):
    refs = list(refs)
    sources = [(refs.pop(0), refs.pop(0)) for _ in plan]
    mix_ref = refs.pop(0)
    if with_router:
        weight_ref, gain_ref = refs.pop(0), refs.pop(0)
    outs = [refs.pop(0) for _ in plan]
    if with_router:
        router_ref = refs.pop(0)
    w_buf, avg_buf, share_buf, in_sem, share_sem, send_sem, recv_sem = refs[:7]
    if with_router:
        weight_buf, gain_buf, stage, total, small_sem, hop_send, hop_recv, row_send, row_recv = refs[7:]
    me, at = lax.axis_index("shard"), lax.axis_index("expert")
    experts, depth, width = sources[0][0].shape
    per = (width if BY_COLUMN else depth) // size
    counts = [(last - first) * per for first, last, _ in plan]

    def load(m, i):
        slot = lax.rem(i, SLOTS)
        expert, start = plan[m][0] + lax.div(i, per), pl.multiple_of(lax.rem(i, per) * size, size)
        def part(src):
            return src.at[expert, :, pl.ds(start, size)] if BY_COLUMN else src.at[expert, pl.ds(start, size), :]
        return [
            pltpu.make_async_copy(part(src), buf.at[slot], in_sem.at[n, slot])
            for n, (src, buf) in enumerate(zip(sources[m], (w_buf, avg_buf)))
        ]

    def block(m, i, owner):
        expert, start = lax.div(i, per), lax.rem(i, per) * size
        base = owner * depth if plan[m][2] else 0
        if BY_COLUMN:
            column = pl.multiple_of(base, depth) if plan[m][2] else 0
            return outs[m].at[expert, pl.ds(pl.multiple_of(start, size), size), pl.ds(column, depth)]
        return outs[m].at[expert, :, pl.ds(pl.multiple_of(base + start, size), size)]

    def exchange(m, i, owner, k):
        at_sem = sum(c for c, p in zip(counts[:m], plan) if p[2]) + i
        return pltpu.make_async_remote_copy(
            src_ref=block(m, i, owner), dst_ref=block(m, i, owner),
            send_sem=send_sem.at[k - 1, at_sem], recv_sem=recv_sem.at[k - 1, at_sem],
            device_id={"shard": lax.rem(me + k, shards)}, device_id_type=MESH,
        )

    for i in range(SLOTS):
        for copy in load(0, i):
            copy.start()
    if experts > 1:
        share_copy = pltpu.make_async_copy(mix_ref, share_buf, share_sem)
        share_copy.start()
    if with_router:
        small = [
            pltpu.make_async_copy(weight_ref, weight_buf, small_sem.at[0]),
            pltpu.make_async_copy(gain_ref, gain_buf, small_sem.at[1]),
        ]
        for copy in small:
            copy.start()

    barrier = pltpu.get_barrier_semaphore()
    for k in range(1, shards):
        pl.semaphore_signal(barrier, inc=1, device_id={"shard": lax.rem(me + k, shards)}, device_id_type=MESH)
    if with_router:
        @pl.loop(1, peers)
        def _(k):
            pl.semaphore_signal(barrier, inc=1, device_id={"expert": lax.rem(at + k, peers)}, device_id_type=MESH)
    pl.semaphore_wait(barrier, shards - 1 + (peers - 1 if with_router else 0))

    if with_router:
        mine = pl.ds(pl.multiple_of(me * depth, depth), depth)
        for copy in small:
            copy.wait()
        stage[at, :, mine] = (weight_buf[...] * gain_buf[...]).astype(jnp.bfloat16)

        def hop(k):
            return pltpu.make_async_remote_copy(
                src_ref=stage.at[at, :, mine], dst_ref=stage.at[at, :, mine],
                send_sem=hop_send.at[k - 1], recv_sem=hop_recv.at[k - 1],
                device_id={"expert": lax.rem(at + k, peers)}, device_id_type=MESH,
            )

        def hop_in(k):
            source = lax.rem(at + peers - k, peers)
            return pltpu.make_async_remote_copy(
                src_ref=stage.at[source, :, mine], dst_ref=stage.at[source, :, mine],
                send_sem=hop_send.at[k - 1], recv_sem=hop_recv.at[k - 1],
                device_id={"expert": lax.rem(at + k, peers)}, device_id_type=MESH,
            )

        @pl.loop(1, peers)
        def _(k):
            hop(k).start()

        def rows_to(owner, k):
            columns = pl.ds(pl.multiple_of(owner * depth, depth), depth)
            return pltpu.make_async_remote_copy(
                src_ref=stage.at[:, :, columns], dst_ref=stage.at[:, :, columns],
                send_sem=row_send.at[k - 1], recv_sem=row_recv.at[k - 1],
                device_id={"shard": lax.rem(me + k, shards)}, device_id_type=MESH,
            )

        def pass_on():
            @pl.loop(1, peers)
            def _(k):
                hop(k).wait_send()
                hop_in(k).wait_recv()

            for k in range(1, shards):
                rows_to(me, k).start()

    if experts > 1:
        share_copy.wait()
    shares = share_buf if experts > 1 else mix_ref

    for m, (first, last, sends) in enumerate(plan):
        @pl.loop(0, counts[m])
        def _(i):
            slot = lax.rem(i, SLOTS)
            for copy in load(m, i):
                copy.wait()
            share = shares[first + lax.div(i, per)]
            fresh = share * w_buf[slot] + (1.0 - share) * avg_buf[slot]
            block(m, i, me)[...] = jnp.transpose(fresh.astype(jnp.bfloat16))
            if sends:
                for k in range(1, shards):
                    exchange(m, i, me, k).start()

            if with_router and m == 0:
                pl.when(i == counts[0] // 2)(pass_on)

            @pl.when(i + SLOTS < counts[m])
            def _():
                for copy in load(m, i + SLOTS):
                    copy.start()

            if m + 1 < len(plan):
                @pl.when(i + SLOTS >= counts[m])
                def _():
                    for copy in load(m + 1, i + SLOTS - counts[m]):
                        copy.start()

    if with_router:
        for k in range(1, shards):
            rows_to(me, k).wait_send()
            rows_to(lax.rem(me + shards - k, shards), k).wait_recv()
        held = stage.shape[1]
        for e in range(peers):
            total[e * held:(e + 1) * held, :] = stage[e].astype(jnp.float32)
        router_ref[...] = total[...].astype(jnp.bfloat16)

    for m, (_, _, sends) in enumerate(plan):
        if sends:
            @pl.loop(0, counts[m])
            def _(i):
                for k in range(1, shards):
                    exchange(m, i, me, k).wait_send()
                    exchange(m, i, lax.rem(me + shards - k, shards), k).wait_recv()


def mix(mesh, plan, sources, share, number, router=None):
    peers, shards = mesh.shape["expert"], mesh.shape["shard"]
    experts, depth, width = sources[0].shape
    span = width if BY_COLUMN else depth
    size = min(SIZE, span)
    per = span // size
    assert per % SLOTS == 0
    pieces = sum((last - first) * per for first, last, sends in plan if sends)
    others = max(shards - 1, 1)
    hbm_spec = pl.BlockSpec(memory_space=pltpu.HBM)
    vmem_spec = pl.BlockSpec(memory_space=pltpu.VMEM)
    buffer = pltpu.VMEM((SLOTS, depth, size) if BY_COLUMN else (SLOTS, size, width), jnp.float32)
    out_shape = [
        pltpu.VMEM((last - first, width, (shards if sends else 1) * depth), jnp.bfloat16)
        for first, last, sends in plan
    ]
    share_spec = hbm_spec if experts > 1 else pl.BlockSpec(memory_space=pltpu.SMEM)
    in_specs = [hbm_spec] * len(sources) + [share_spec]
    scratch = [
        buffer,
        buffer,
        pltpu.SMEM(share.shape, jnp.float32),
        pltpu.SemaphoreType.DMA((2, SLOTS)),
        pltpu.SemaphoreType.DMA,
        pltpu.SemaphoreType.DMA((others, pieces)),
        pltpu.SemaphoreType.DMA((others, pieces)),
    ]
    far = functools.partial(pltpu.with_memory_space_constraint, memory_space=pltpu.HBM)
    args = [far(x) for x in sources] + [far(share) if experts > 1 else share]
    if router is not None:
        args += [far(x) for x in router]
        in_specs += [hbm_spec, hbm_spec]
        out_shape += [pltpu.VMEM((peers * experts, shards * depth), jnp.bfloat16)]
        scratch += [
            pltpu.VMEM(router[0].shape, jnp.float32),
            pltpu.VMEM(router[1].shape, jnp.float32),
            pltpu.VMEM((peers, experts, shards * depth), jnp.bfloat16),
            pltpu.VMEM((peers * experts, shards * depth), jnp.float32),
            pltpu.SemaphoreType.DMA((2,)),
            pltpu.SemaphoreType.DMA((peers,)),
            pltpu.SemaphoreType.DMA((peers,)),
            pltpu.SemaphoreType.DMA((others,)),
            pltpu.SemaphoreType.DMA((others,)),
        ]
    moved = sum((last - first) * depth * width * 8 for first, last, _ in plan)
    return pl.pallas_call(
        functools.partial(mix_kernel, peers, shards, size, plan, router is not None),
        out_shape=out_shape,
        in_specs=in_specs,
        out_specs=[vmem_spec] * len(out_shape),
        scratch_shapes=scratch,
        cost_estimate=pl.CostEstimate(flops=0, bytes_accessed=moved, transcendentals=0),
        compiler_params=pltpu.CompilerParams(
            collective_id=number, has_side_effects=True, vmem_limit_bytes=12 * 2**20
        ),
    )(*args)


def store_kernel(place, *refs):
    copies = [
        pltpu.make_async_copy(source, target, refs[-1].at[n])
        for n, (source, target) in enumerate(place(*refs[:-1]))
    ]
    for copy in copies:
        copy.start()
    for copy in copies:
        copy.wait()


def store(place, count, shapes, *arrays):
    vmem_spec = pl.BlockSpec(memory_space=pltpu.VMEM)
    moved = sum(x.size * x.dtype.itemsize for x in arrays)
    return pl.pallas_call(
        functools.partial(store_kernel, place),
        out_shape=[pltpu.HBM(x.shape, x.dtype) for x in shapes],
        in_specs=[vmem_spec] * len(arrays),
        out_specs=[pl.BlockSpec(memory_space=pltpu.HBM)] * len(shapes),
        scratch_shapes=[pltpu.SemaphoreType.DMA((count,))],
        cost_estimate=pl.CostEstimate(flops=0, bytes_accessed=2 * moved, transcendentals=0),
        compiler_params=pltpu.CompilerParams(vmem_limit_bytes=2**20),
    )(*arrays)


def solution(mesh):
    shards = mesh.shape["shard"]

    def local(w_gate, avg_gate, w_up, avg_up, mix_share, router_weight, router_gain):
        experts, depth, width = w_gate.shape
        early = experts // EARLY
        whole = jax.ShapeDtypeStruct((experts, width, shards * depth), jnp.bfloat16)
        plan, sources = [(0, experts, True)], [w_gate, avg_gate]
        if early:
            plan, sources = plan + [(0, early, False)], sources + [w_up, avg_up]
        halves = list(mix(mesh, plan, sources, mix_share, 0))
        held = [
            lax.ppermute(halves[1], "shard", [(n, (n + k) % shards) for n in range(shards)])
            for k in range(1, shards)
        ] if early else []

        def place_gate(gate, gate_out):
            return [(gate.at[e], gate_out.at[e]) for e in range(experts)]

        gate, = store(place_gate, experts, (whole,), halves[0])
        mix_share, gate = lax.optimization_barrier((mix_share, gate))
        late, router = mix(
            mesh, [(early, experts, True)], [w_up, avg_up], mix_share, 1,
            [router_weight.T, router_gain[None, :]],
        )

        def place_up(late, router, *rest):
            *parts, out, router_out = rest
            me = lax.axis_index("shard")
            moves = [(router, router_out)] + [(late.at[e], out.at[early + e]) for e in range(experts - early)]
            for k, part in enumerate(parts):
                owner = lax.rem(me + shards - k, shards)
                column = pl.ds(pl.multiple_of(owner * depth, depth), depth)
                moves += [(part.at[e], out.at[e, :, column]) for e in range(early)]
            return moves

        parts = halves[1:] + held
        count = experts - early + early * len(parts) + 1
        up, router = store(place_up, count, (whole, router), late, router, *parts)
        return gate, up, router.T

    return jax.shard_map(
        local,
        mesh=mesh,
        in_specs=(
            P("expert", "shard", None),
            P("expert", "shard", None),
            P("expert", "shard", None),
            P("expert", "shard", None),
            P("expert"),
            P("shard", "expert"),
            P("shard"),
        ),
        out_specs=(P("expert", None, None), P("expert", None, None), P()),
        check_vma=False,
    )
```
